32 devices in a mesh: seq: 8 (over y, x, core), head: 4 (over z).
Axes of the slice: x: 2, y: 2, z: 4, core: 2. Of those that a mesh axis runs over, the one named last changes fastest.
Arguments:
- latent: bfloat16 [8, 1024, 2048], P('seq', None, 'head'), may hold values from -6 to 6
- modulation: float32 [9, 2048], replicated, may hold values from -3 to 3
- spatial_qkv: bfloat16 [3, 2048, 2048], P(None, None, 'head')
- spatial_out: bfloat16 [2048, 2048], P('head'), may hold values from -0.125 to 0.125
- temporal_qkv: bfloat16 [3, 2048, 2048], P(None, None, 'head')
- temporal_out: bfloat16 [2048, 2048], P('head'), may hold values from -0.125 to 0.125
- hidden_weight: bfloat16 [2048, 8192], P(None, 'head'), may hold values from -0.125 to 0.125
- output_weight: bfloat16 [8192, 2048], P('head'), may hold values from -0.0625 to 0.0625
Outputs:
- block_out: bfloat16 [8, 1024, 2048], P(None, 'seq', 'head')
The draws below stay inside these ranges and needn't reach their ends.
All inputs are finite; a program needn't handle non-finite values.
Results may differ from the reference program's by a relative error of at most 0.009.
Values may be sent and summed in bfloat16 or wider, within the bound.
A program may use at most 128 MiB of HBM per device.

```python
import jax
import jax.numpy as jnp
from jax import lax

D = 2048
HEADS = 32
FF = 8192
P_SIZE = 1024
HD = 64
FRAMES = 8


def projection_draw(key, salt):
    key = jax.random.fold_in(key, salt)
    first, second, third = jax.random.split(key, 3)
    spread = D ** (-0.5)
    query = jax.random.normal(first, (D, D), jnp.float32) * spread
    keys = jax.random.normal(second, (D, D), jnp.float32) * spread
    values = jax.random.normal(third, (D, D), jnp.float32) * spread
    return jnp.stack([query, keys, values]).astype(jnp.bfloat16)


def draw_spatial_qkv(key, part):
    return projection_draw(key, 11)


def draw_temporal_qkv(key, part):
    return projection_draw(key, 23)


def level_of(rng, extent, cuts, least, high):
    factor_of = 1.0
    for dim, parts in cuts:
        draws = jax.random.uniform(jax.random.fold_in(jax.random.fold_in(rng, 6), dim), (parts,), jnp.float32, least / len(cuts), high / len(cuts))
        factor_of = factor_of * jnp.repeat(jnp.exp(draws), extent[dim] // parts).reshape((-1,) + (1,) * (len(extent) - 1 - dim))
    return factor_of


def normal_values(stream_key, shape, scale, most, cuts=(), kind=jnp.bfloat16):
    drawn = jax.random.normal(stream_key, shape, jnp.float32) * scale
    if len(cuts) > 0:
        drawn = level_of(stream_key, shape, cuts, -0.22, 0.18) * drawn
    return jnp.clip(drawn, min=-most, max=most).astype(kind)


def setup_inputs(seed: int = 0) -> dict:
    arg_keys = jax.random.split(jax.random.key(seed), 9)
    return {
        "latent": normal_values(arg_keys[0], (FRAMES, P_SIZE, D), 1.0, 6.0, ((0, 8), (2, 4))),
        "modulation": normal_values(arg_keys[1], (9, D), 0.5, 3.0, (), jnp.float32),
        "spatial_qkv": draw_spatial_qkv(jax.random.fold_in(arg_keys[8], 71), 0),
        "spatial_out": normal_values(arg_keys[3], (D, D), D ** -0.5, 0.125, ((0, 4),)),
        "temporal_qkv": draw_temporal_qkv(jax.random.fold_in(arg_keys[8], 71), 0),
        "temporal_out": normal_values(arg_keys[5], (D, D), D ** -0.5, 0.125, ((0, 4),)),
        "hidden_weight": normal_values(arg_keys[6], (D, FF), D ** -0.5, 0.125, ((1, 4),)),
        "output_weight": normal_values(arg_keys[7], (FF, D), FF ** -0.5, 0.0625, ((0, 4),)),
    }


def layer_norm(values):
    average = lax.optimization_barrier(jnp.mean(values, axis=-1, keepdims=True))
    centred = values - average
    variance = lax.optimization_barrier(jnp.mean(centred * centred, axis=-1, keepdims=True))
    return centred * lax.rsqrt(variance + 1e-06)

def modulate(stream, modulation, offset):
    normed = layer_norm(stream.astype(jnp.float32))
    return (normed * (1.0 + modulation[offset + 1]) + modulation[offset]).astype(jnp.bfloat16)

def attend(query, keys, values):
    scores = jnp.einsum('glhd,gmhd->ghlm', query.astype(jnp.float32), keys.astype(jnp.float32)) * HD ** (-0.5)
    attn_weights = jax.nn.softmax(scores, axis=-1).astype(jnp.bfloat16)
    return jnp.einsum('ghlm,gmhd->glhd', attn_weights.astype(jnp.float32), values.astype(jnp.float32)).astype(jnp.bfloat16)

def project_three(normed, weights):
    return [jnp.dot(normed, weights[member], preferred_element_type=jnp.float32).astype(jnp.bfloat16) for member in range(3)]

def reference(latent, modulation, spatial_qkv, spatial_out, temporal_qkv, temporal_out, hidden_weight, output_weight):
    frames = latent.shape[0]
    patches = latent.shape[1]

    def split_heads(tensor):
        return tensor.reshape(frames, patches, HEADS, HD)
    normed = modulate(latent, modulation, 0)
    query, keys, values = [split_heads(member) for member in project_three(normed, spatial_qkv)]
    spatial = lax.map(lambda triple: attend(triple[0][None], triple[1][None], triple[2][None])[0], (query, keys, values))
    spatial = spatial.reshape(frames, patches, D)
    branch = jnp.dot(spatial, spatial_out, preferred_element_type=jnp.float32)
    stream_one = (latent.astype(jnp.float32) + modulation[2] * branch).astype(jnp.bfloat16)
    normed = modulate(stream_one, modulation, 3)
    query, keys, values = [jnp.transpose(split_heads(member), (1, 0, 2, 3)) for member in project_three(normed, temporal_qkv)]
    temporal = jnp.transpose(attend(query, keys, values), (1, 0, 2, 3)).reshape(frames, patches, D)
    branch = jnp.dot(temporal, temporal_out, preferred_element_type=jnp.float32)
    stream_two = (stream_one.astype(jnp.float32) + modulation[5] * branch).astype(jnp.bfloat16)
    normed = modulate(stream_two, modulation, 6)
    hidden = jax.nn.gelu(jnp.dot(normed, hidden_weight, preferred_element_type=jnp.float32), approximate=True).astype(jnp.bfloat16)
    branch = jnp.dot(hidden, output_weight, preferred_element_type=jnp.float32)
    return (stream_two.astype(jnp.float32) + modulation[8] * branch).astype(jnp.bfloat16)
```

```python
import functools
import math

import jax
import jax.numpy as jnp
from jax import lax
from jax.experimental import pallas as pl
from jax.experimental.pallas import tpu as pltpu
from jax.sharding import PartitionSpec as P

HD = 64
PAIR = 128
CHUNKS = 4
AHEAD = 2
EXP2_SCALE = HD ** (-0.5) * math.log2(math.e)
GELU_SCALE = math.sqrt(2.0 / math.pi)
BF16 = jnp.bfloat16
F32 = jnp.float32
NT = (((1,), (1,)), ((), ()))
VMEM_LIMIT = 60 * 1024 * 1024
DMA = pltpu.SemaphoreType.DMA


def weighted_values(scores, values):
    top = jnp.max(scores, axis=-1, keepdims=True)
    weights = jnp.exp2((scores - top) * EXP2_SCALE).astype(BF16)
    extended = jnp.concatenate([values, jnp.ones_like(values)], axis=1)
    summed = jnp.dot(weights, extended, preferred_element_type=F32)
    return summed[:, :HD] / summed[:, HD:]


def gelu(x):
    return 0.5 * x * (1.0 + jnp.tanh(GELU_SCALE * (x + 0.044715 * (x * x * x))))


class Line:
    def __init__(self, n, gathered, partial, below, above, sems):
        self.n = n
        self.z = lax.axis_index("head")
        self.gathered, self.partial = gathered, partial
        self.below, self.above = below, above
        self.got, self.gave, self.from_below, self.from_above, self.passed = sems

    def barrier(self):
        sem = pltpu.get_barrier_semaphore()
        has_lower, has_upper = self.z > 0, self.z < self.n - 1

        @pl.when(has_lower)
        def _():
            pl.semaphore_signal(sem, inc=1, device_id={"head": self.z - 1})

        @pl.when(has_upper)
        def _():
            pl.semaphore_signal(sem, inc=1, device_id={"head": self.z + 1})

        pl.semaphore_wait(sem, has_lower.astype(jnp.int32) + has_upper.astype(jnp.int32))

    def piece(self, chunk, part, up):
        return pltpu.make_async_remote_copy(
            src_ref=self.gathered.at[chunk, part],
            dst_ref=self.gathered.at[chunk, part],
            send_sem=self.gave.at[0 if up else 1, chunk, part],
            recv_sem=self.got.at[chunk, part],
            device_id={"head": self.z + 1 if up else self.z - 1},
        )

    def give(self, chunk, part):
        @pl.when(self.z < self.n - 1)
        def _():
            self.piece(chunk, part, True).start()

        @pl.when(self.z > 0)
        def _():
            self.piece(chunk, part, False).start()

    def collect(self, chunk):
        z, n = self.z, self.n
        for step in range(1, n):

            @pl.when(z - step >= 0)
            def _():
                self.piece(chunk, z - step, True).wait_recv()

                @pl.when(z < n - 1)
                def _():
                    self.piece(chunk, z - step, True).start()

            @pl.when(z + step <= n - 1)
            def _():
                self.piece(chunk, z + step, False).wait_recv()

                @pl.when(z > 0)
                def _():
                    self.piece(chunk, z + step, False).start()

    def total(self, chunk, part, up):
        return pltpu.make_async_remote_copy(
            src_ref=self.partial.at[chunk, part],
            dst_ref=(self.below if up else self.above).at[chunk, part],
            send_sem=self.passed.at[chunk, part],
            recv_sem=(self.from_below if up else self.from_above).at[chunk, part],
            device_id={"head": self.z + 1 if up else self.z - 1},
        )

    def pass_on(self, chunk, lag):
        n = self.n

        def forward(part, up):
            if lag > 0:
                self.total(chunk, part, up).wait_recv()
                came = self.below if up else self.above
                self.partial[chunk, part] = (
                    self.partial[chunk, part].astype(F32) + came[chunk, part].astype(F32)
                ).astype(BF16)
            self.total(chunk, part, up).start()

        @pl.when(self.z == lag)
        def _():
            for part in range(n - 1, lag, -1):
                forward(part, True)

        @pl.when(self.z == n - 1 - lag)
        def _():
            for part in range(n - 1 - lag):
                forward(part, False)

    def finish(self, chunk, acc):
        z = self.z
        acc[...] = self.partial[chunk, z].astype(F32)

        @pl.when(z > 0)
        def _():
            self.total(chunk, z, True).wait_recv()
            acc[...] += self.below[chunk, z].astype(F32)

        @pl.when(z < self.n - 1)
        def _():
            self.total(chunk, z, False).wait_recv()
            acc[...] += self.above[chunk, z].astype(F32)

    def drain(self, chunk):
        z, n = self.z, self.n
        for part in range(n):

            @pl.when((z < n - 1) & (part <= z))
            def _():
                self.piece(chunk, part, True).wait_send()

            @pl.when((z > 0) & (part >= z))
            def _():
                self.piece(chunk, part, False).wait_send()

            @pl.when(part > z)
            def _():
                self.total(chunk, part, True).wait_send()

            @pl.when(part < z)
            def _():
                self.total(chunk, part, False).wait_send()


def normalise(gathered, chunk, mod, normed):
    n, rows, width = gathered.shape[1:]
    group = min(16, rows)

    def body(index, carry):
        here = pl.ds(pl.multiple_of(index * group, group), group)
        parts = [gathered[chunk, part, here, :].astype(F32) for part in range(n)]
        scale = 1.0 / (n * width)
        average = sum(jnp.sum(p, axis=-1, keepdims=True) for p in parts) * scale
        parts = [p - average for p in parts]
        variance = sum(jnp.sum(p * p, axis=-1, keepdims=True) for p in parts) * scale
        factor = lax.rsqrt(variance + 1e-06)
        for part in range(n):
            lanes = slice(part * width, (part + 1) * width)
            normed[here, lanes] = (
                parts[part] * factor * (1.0 + mod[1:2, lanes]) + mod[0:1, lanes]
            ).astype(BF16)
        return carry

    lax.fori_loop(0, rows // group, body, 0)


def project(source, weight, store, tile):
    columns = weight.shape[1]

    def body(index, carry):
        lanes = pl.ds(pl.multiple_of(index * tile, tile), tile)
        store(index, lanes, jnp.dot(source[...], weight[:, lanes], preferred_element_type=F32))
        return carry

    lax.fori_loop(0, columns // tile, body, 0)


def run_stage(line, chunks, x, out, mod, gate, acc, load_sem, weights, first, second):
    n, z = line.n, line.z
    gathered = line.gathered
    rows, width = gathered.shape[2:]
    frames = x.shape[0]
    piece = rows // frames

    def own(chunk, frame):
        return pltpu.make_async_copy(
            x.at[frame, pl.ds(pl.multiple_of(chunk * piece, piece), piece), :],
            gathered.at[chunk, z, pl.ds(frame * piece, piece), :],
            load_sem.at[chunk, frame],
        )

    for chunk in range(chunks):
        for frame in range(frames):
            own(chunk, frame).start()
    for copy in weights:
        copy.start()
    line.barrier()
    for chunk in range(chunks):
        for frame in range(frames):
            own(chunk, frame).wait()
        if chunk < AHEAD:
            line.give(chunk, z)

    def arrive(chunk):
        line.collect(chunk)

        @pl.when(chunk + AHEAD < chunks)
        def _():
            line.give(chunk + AHEAD, z)

    def pass_older(step):
        for lag in range(n - 1, 0, -1):
            chunk = step - lag

            @pl.when((chunk >= 0) & (chunk < chunks))
            def _():
                line.pass_on(chunk, lag)

    def complete(chunk):
        line.finish(chunk, acc)
        total = gathered[chunk, z].astype(F32) + gate[...] * acc[...]
        here = pl.ds(pl.multiple_of(chunk * piece, piece), piece)
        out[:, here, :] = total.astype(BF16).reshape(frames, piece, width)

    if first is not None:

        def gather_step(step, carry):
            arrive(step)

            @pl.when(step == 0)
            def _():
                for copy in weights:
                    copy.wait()

            first(step)
            return carry

        lax.fori_loop(0, chunks, gather_step, 0)

    def main_step(step, carry):
        if first is None:

            @pl.when(step < chunks)
            def _():
                arrive(step)

        pass_older(step)

        @pl.when(step < chunks)
        def _():
            if first is None:

                @pl.when(step == 0)
                def _():
                    for copy in weights:
                        copy.wait()

            second(step)
            line.pass_on(step, 0)

        @pl.when(step >= n - 1)
        def _():
            complete(step - (n - 1))

        return carry

    lax.fori_loop(0, chunks + n - 1, main_step, 0)

    def drain(chunk, carry):
        line.drain(chunk)
        return carry

    lax.fori_loop(0, chunks, drain, 0)


def spatial_kernel(n, chunks, x, w_in, w_out, mod, gate, out, gathered, partial, below, above, *rest):
    *sems, load_sem, w_sem, acc, normed, w_in_v, w_out_v, query, keys, values, mixed = rest
    line = Line(n, gathered, partial, below, above, sems)
    rows, width = gathered.shape[2:]
    weights = [
        pltpu.make_async_copy(w_in, w_in_v, w_sem.at[0]),
        pltpu.make_async_copy(w_out, w_out_v, w_sem.at[1]),
    ]

    def first(chunk):
        normalise(gathered, chunk, mod, normed)
        here = pl.ds(pl.multiple_of(chunk * rows, rows), rows)
        for member, target in enumerate((query, keys, values)):
            target[here, :] = jnp.dot(
                normed[...], w_in_v[member], preferred_element_type=F32
            ).astype(BF16)

    def second(chunk):
        here = pl.ds(pl.multiple_of(chunk * rows, rows), rows)

        def pair(index, carry):
            lanes = pl.ds(pl.multiple_of(index * PAIR, PAIR), PAIR)
            q, k, v = query[here, lanes], keys[:, lanes], values[:, lanes]
            outs = []
            for head in range(PAIR // HD):
                mine = slice(head * HD, (head + 1) * HD)
                scores = lax.dot_general(q[:, mine], k[:, mine], NT, preferred_element_type=F32)
                outs.append(weighted_values(scores, v[:, mine]))
            mixed[:, lanes] = jnp.concatenate(outs, axis=1).astype(BF16)
            return carry

        lax.fori_loop(0, width // PAIR, pair, 0)

        def store(index, lanes, value):
            partial[chunk, index] = value.astype(BF16)

        project(mixed, w_out_v, store, width)

    run_stage(line, chunks, x, out, mod, gate, acc, load_sem, weights, first, second)


def temporal_kernel(n, chunks, x, w_in, w_out, mod, gate, out, gathered, partial, below, above, *rest):
    *sems, load_sem, w_sem, acc, normed, w_in_v, w_out_v, query, keys, values, mixed = rest
    line = Line(n, gathered, partial, below, above, sems)
    rows, width = gathered.shape[2:]
    frames = x.shape[0]
    patches = rows // frames
    group = min(128 // frames, patches)
    weights = [
        pltpu.make_async_copy(w_in, w_in_v, w_sem.at[0]),
        pltpu.make_async_copy(w_out, w_out_v, w_sem.at[1]),
    ]

    def second(chunk):
        normalise(gathered, chunk, mod, normed)
        for member, target in enumerate((query, keys, values)):
            value = jnp.dot(normed[...], w_in_v[member], preferred_element_type=F32)
            target[...] = value.astype(BF16).reshape(frames, patches, width)
        size = frames * group
        row = lax.broadcasted_iota(jnp.int32, (size, size), 0)
        column = lax.broadcasted_iota(jnp.int32, (size, size), 1)
        same_patch = lax.rem(row, group) == lax.rem(column, group)
        for start in range(0, patches, group):
            here = slice(start, start + group)

            def pair(index, carry):
                lanes = pl.ds(pl.multiple_of(index * PAIR, PAIR), PAIR)
                q, k, v = [
                    source[:, here, lanes].reshape(size, PAIR) for source in (query, keys, values)
                ]
                outs = []
                for head in range(PAIR // HD):
                    mine = slice(head * HD, (head + 1) * HD)
                    scores = lax.dot_general(
                        q[:, mine], k[:, mine], NT, preferred_element_type=F32
                    )
                    outs.append(
                        weighted_values(jnp.where(same_patch, scores, -jnp.inf), v[:, mine])
                    )
                mixed[:, here, lanes] = (
                    jnp.concatenate(outs, axis=1).astype(BF16).reshape(frames, group, PAIR)
                )
                return carry

            lax.fori_loop(0, width // PAIR, pair, 0)
        source = mixed[...].reshape(rows, width)

        def body(index, carry):
            lanes = pl.ds(pl.multiple_of(index * width, width), width)
            partial[chunk, index] = jnp.dot(
                source, w_out_v[:, lanes], preferred_element_type=F32
            ).astype(BF16)
            return carry

        lax.fori_loop(0, n, body, 0)

    run_stage(line, chunks, x, out, mod, gate, acc, load_sem, weights, None, second)


def mlp_kernel(n, chunks, x, w_in, w_out, mod, gate, out, gathered, partial, below, above, *rest):
    *sems, load_sem, w_sem, acc, normed, w_in_v, w_out_v, hidden = rest
    line = Line(n, gathered, partial, below, above, sems)
    width = gathered.shape[3]
    weights = [
        pltpu.make_async_copy(w_in, w_in_v, w_sem.at[0]),
        pltpu.make_async_copy(w_out, w_out_v, w_sem.at[1]),
    ]

    def second(chunk):
        normalise(gathered, chunk, mod, normed)

        def keep(index, lanes, value):
            hidden[:, lanes] = gelu(value).astype(BF16)

        project(normed, w_in_v, keep, min(512, w_in_v.shape[1]))

        def store(index, lanes, value):
            partial[chunk, index] = value.astype(BF16)

        project(hidden, w_out_v, store, width)

    run_stage(line, chunks, x, out, mod, gate, acc, load_sem, weights, None, second)


def stage(kernel, name, number, x, w_in, w_out, mod, gate, extra, flops):
    n = lax.axis_size("head")
    frames, patches, width = x.shape
    chunks = CHUNKS
    rows = frames * patches // chunks
    model = n * width
    store = pltpu.VMEM((chunks, n, rows, width), BF16)
    any_space = pl.BlockSpec(memory_space=pl.ANY)
    vmem = pl.BlockSpec(memory_space=pltpu.VMEM)
    return pl.pallas_call(
        functools.partial(kernel, n, chunks),
        out_shape=jax.ShapeDtypeStruct(x.shape, BF16),
        in_specs=[any_space, any_space, any_space, vmem, vmem],
        out_specs=vmem,
        scratch_shapes=[
            store,
            store,
            store,
            store,
            DMA((chunks, n)),
            DMA((2, chunks, n)),
            DMA((chunks, n)),
            DMA((chunks, n)),
            DMA((chunks, n)),
            DMA((chunks, frames)),
            DMA((2,)),
            pltpu.VMEM((rows, width), F32),
            pltpu.VMEM((rows, model), BF16),
            pltpu.VMEM(w_in.shape, BF16),
            pltpu.VMEM(w_out.shape, BF16),
        ]
        + extra(rows),
        compiler_params=pltpu.CompilerParams(
            collective_id=number, has_side_effects=True, vmem_limit_bytes=VMEM_LIMIT
        ),
        cost_estimate=pl.CostEstimate(
            flops=flops, bytes_accessed=4 * x.size + 2 * (w_in.size + w_out.size), transcendentals=0
        ),
        name=name,
    )(x, w_in, w_out, mod, gate)


def per_device(
    latent,
    modulation,
    spatial_qkv,
    spatial_out,
    temporal_qkv,
    temporal_out,
    hidden_weight,
    output_weight,
):
    frames_local, patches, width = latent.shape
    seq = lax.axis_size("seq")
    part = patches // seq
    anchor = lax.axis_index("head") * width
    gates = lax.dynamic_slice_in_dim(modulation, anchor, width, 1)
    tokens = frames_local * patches

    def spatial_extra(rows):
        whole = pltpu.VMEM((tokens, width), BF16)
        return [whole, whole, whole, pltpu.VMEM((rows, width), BF16)]

    def temporal_extra(rows):
        frames = frames_local * seq
        return [pltpu.VMEM((frames, rows // frames, width), BF16)] * 4

    def mlp_extra(rows):
        return [pltpu.VMEM((rows, hidden_weight.shape[1]), BF16)]

    model = modulation.shape[1]
    base = 2 * tokens * model
    one = stage(
        spatial_kernel, "spatial", 0, latent.reshape(seq, part, width), spatial_qkv, spatial_out,
        modulation[0:2], gates[2:3], spatial_extra, base * 4 * width,
    )
    one = lax.all_to_all(one, "seq", split_axis=0, concat_axis=0, tiled=True)
    two = stage(
        temporal_kernel, "temporal", 1, one, temporal_qkv, temporal_out,
        modulation[3:5], gates[5:6], temporal_extra, base * 4 * width,
    )
    return stage(
        mlp_kernel, "mlp", 2, two, hidden_weight, output_weight,
        modulation[6:8], gates[8:9], mlp_extra, base * 2 * hidden_weight.shape[1],
    )


def solution(mesh):
    in_specs = (
        P("seq", None, "head"),
        P(),
        P(None, None, "head"),
        P("head", None),
        P(None, None, "head"),
        P("head", None),
        P(None, "head"),
        P("head", None),
    )
    out_specs = P(None, "seq", "head")
    return jax.shard_map(
        per_device, mesh=mesh, in_specs=in_specs, out_specs=out_specs, check_vma=False
    )
```
